256 devices in a mesh: tm: 64 (over z, y, core), freq: 4 (over x).
Axes of the slice: x: 4, y: 4, z: 8, core: 2. Of those that a mesh axis runs over, the one named last changes fastest.
Arguments:
- visibilities: bfloat16 [2, 64, 1024, 1024], P(None, 'freq', 'tm'), may hold values from -6 to 6
- projection: bfloat16 [128, 64, 2, 2, 64, 512], P('tm', 'freq'), may hold values from -0.1875 to 0.1875
- kl_weight: bfloat16 [128, 2, 64, 64], P('tm'), may hold values from -0.5 to 0.5
- azimuthal: int32 [128], replicated, may hold values from 0 to 1023, as said below
- live_mode_totals: int32 [128, 64, 2], P('tm', 'freq'), may hold values from 1 to 64, as said below
Outputs:
- kl_modes: float32 [128, 2, 64, 2, 64], P('tm', None, None, None, 'freq')
The draws below stay inside these ranges and needn't reach their ends.
Inputs may be any that keep to these rules, and one draw needn't show every extreme that they name: `azimuthal`: the m values are distinct. `live_mode_totals`: slots from the count up to 64 are padding; the count 64 occurs in every draw.
All inputs are finite; a program needn't handle non-finite values.
Results may differ from the reference program's by a relative error of at most 0.012.
Values may be sent and summed in bfloat16 or wider, within the bound.
A program may use at most 192 MiB of HBM per device.

```python
import math
import jax
import jax.numpy as jnp
from jax import lax

BL = 512
POL = 2
F = 64
TIMES = 1024
MODES = 64
M = 128


def draw_azimuthal(key, part):
    return jax.random.permutation(key, TIMES)[:M].astype(jnp.int32)


def draw_live_mode_totals(key, part):
    counts = jax.random.randint(key, (M * F * POL,), 1, MODES + 1, dtype=jnp.int32)
    where_full = jax.random.randint(jax.random.fold_in(key, 7), (), 0, M * F * POL, dtype=jnp.int32)
    counts = counts.at[where_full].set(MODES)
    return counts.reshape(M, F, POL)


def levels(stream_key, extent, shards, low, top_value):
    def one(position, shards_of):
        heights = jax.random.uniform(jax.random.fold_in(jax.random.fold_in(stream_key, 6), position), (shards_of,), jnp.float32, low / len(shards), top_value / len(shards))
        return jnp.repeat(jnp.exp(heights), extent[position] // shards_of).reshape((-1,) + (1,) * (len(extent) - position - 1))

    level = one(*shards[0])
    for cut in shards[1:]:
        level = level * one(*cut)
    return level


def gaussian(stream_key, shape, deviation, reach, pieces=(), held_as=jnp.bfloat16):
    entries = jax.random.normal(stream_key, shape, jnp.float32) * deviation
    if len(pieces) > 0:
        entries = levels(stream_key, shape, pieces, -0.22, 0.18) * entries
    return jnp.clip(entries, min=-reach, max=reach).astype(held_as)


def setup_inputs(seed: int = 0) -> dict:
    key_of = jax.random.split(jax.random.key(seed), 6)
    return {
        "visibilities": gaussian(key_of[0], (2, F, TIMES, POL * BL), 1.0, 6.0, ((1, 4), (2, 64))),
        "projection": gaussian(key_of[1], (M, F, POL, 2, MODES, BL), (2 * BL) ** -0.5, 0.1875, ((0, 64), (1, 4))),
        "kl_weight": gaussian(key_of[2], (M, 2, F, F), (2 * F) ** -0.5, 0.5, ((0, 64),)),
        "azimuthal": draw_azimuthal(jax.random.fold_in(key_of[5], 71), 0),
        "live_mode_totals": draw_live_mode_totals(jax.random.fold_in(key_of[5], 71), 0),
    }


def reference(visibilities, projection, kl_weight, azimuthal, live_mode_totals):
    time_index = jnp.arange(TIMES, dtype=jnp.int32)
    phase_index = azimuthal.astype(jnp.int32)[:, None] * time_index[None, :] % TIMES
    angles = phase_index.astype(jnp.float32) * (2.0 * math.pi / TIMES)
    cosine_table = jnp.cos(angles)
    sine_table = jnp.sin(angles)
    norm_factor = 1.0 / math.sqrt(TIMES)
    highest = lax.Precision.HIGHEST

    def per_channel(channel):
        real_part = visibilities[0, channel].astype(jnp.float32)
        imag_part = visibilities[1, channel].astype(jnp.float32)
        out_real = jnp.dot(cosine_table, real_part, precision=highest) + jnp.dot(sine_table, imag_part, precision=highest)
        out_imag = jnp.dot(cosine_table, imag_part, precision=highest) - jnp.dot(sine_table, real_part, precision=highest)
        return jnp.stack([out_real, out_imag], axis=1) * norm_factor
    mode_spectra = lax.map(per_channel, jnp.arange(F, dtype=jnp.int32))
    mode_spectra = jnp.transpose(mode_spectra, (1, 0, 2, 3)).astype(jnp.bfloat16)
    mode_spectra = mode_spectra.reshape(M, F, 2, POL, BL)
    modes_iota = jnp.arange(MODES, dtype=jnp.int32)

    def slot_entries(inputs):
        matrix, vector, counts = inputs
        matrix_f = matrix.astype(jnp.float32)
        vector_f = vector.astype(jnp.float32)

        def apply_map(mat_part, vec_part):
            return jnp.einsum('fpkb,fpb->fpk', mat_part, vec_part)
        proj_real = apply_map(matrix_f[:, :, 0], vector_f[:, 0]) - apply_map(matrix_f[:, :, 1], vector_f[:, 1])
        proj_imag = apply_map(matrix_f[:, :, 0], vector_f[:, 1]) + apply_map(matrix_f[:, :, 1], vector_f[:, 0])
        live_slots = modes_iota[None, None, :] < counts[:, :, None]
        stacked_modes = jnp.stack([proj_real, proj_imag], axis=1)
        return jnp.where(live_slots[:, None], stacked_modes, 0.0).astype(jnp.bfloat16)
    projected = lax.map(slot_entries, (projection, mode_spectra, live_mode_totals))
    weights = kl_weight.astype(jnp.float32)
    values = projected.astype(jnp.float32)

    def kl_mix(weight_part, value_part):
        return jnp.einsum('sgc,scpk->sgpk', weight_part, value_part)
    mixed_real = kl_mix(weights[:, 0], values[:, :, 0]) - kl_mix(weights[:, 1], values[:, :, 1])
    mixed_imag = kl_mix(weights[:, 0], values[:, :, 1]) + kl_mix(weights[:, 1], values[:, :, 0])
    return jnp.stack([mixed_real, mixed_imag], axis=1)
```

```python
import functools
import math

import jax
import jax.numpy as jnp
from jax import lax
from jax.experimental import pallas as pl
from jax.experimental.pallas import tpu as pltpu
from jax.sharding import PartitionSpec as P

MESH = pl.DeviceIdType.MESH
F32 = jnp.float32
BF16 = jnp.bfloat16

ZN = 8
GN = 8
XN = 4
NC = 4
CC = 4
SENDS = ((1, 0), (3, 0), (2, 0), (0, 1), (1, 1), (3, 1), (2, 1))


def iota(shape, dim):
    return lax.broadcasted_iota(jnp.int32, shape, dim)


def cosine_of(phase):
    angle = (jnp.abs(phase - 512) - 256).astype(F32) * (2.0 * math.pi / 1024)
    square = angle * angle
    series = F32(1.0 / math.factorial(13))
    for order in (11, 9, 7, 5, 3, 1):
        sign = 1.0 if (order // 2) % 2 == 0 else -1.0
        series = series * square + F32(sign / math.factorial(order))
    return series * angle


def kernel(
    vis, proj, kl, az, live, out,
    vis_v, streams, proj_v, table, partial, b_send, b_recv, final, c_send, c_recv, d_recv, klw, mixed,
    load_sem, self_sem, proj_sem, a_ssem, a_rsem, b_ssem, b_rsem, c_ssem, c_rsem, d_ssem, d_rsem,
):
    tm = lax.axis_index("tm")
    x = lax.axis_index("freq")
    z = tm // GN
    g = lax.rem(tm, GN)
    y = g // 2
    core = lax.rem(g, 2)

    def in_plane(dy, dc):
        return lax.rem(y + dy, 4) * 2 + lax.rem(core + dc, 2)

    def plane_device(peer):
        return (z * GN + peer, x)

    def z_device(dz):
        return (lax.rem(z + dz + ZN, ZN) * GN + g, x)

    def x_peer(dx):
        return lax.rem(x + dx, XN)

    peers = [in_plane(dy, dc) for dy, dc in SENDS]
    others = [plane_device(peer) for peer in peers]
    others += [z_device(1), z_device(-1)]
    others += [(tm, x_peer(dx)) for dx in (1, 2, 3)]

    barrier = pltpu.get_barrier_semaphore()
    for device in others:
        pl.semaphore_signal(barrier, inc=1, device_id=device, device_id_type=MESH)

    def load(slot, block):
        columns = pl.ds(pl.multiple_of(block * 128, 128), 128)
        return pltpu.make_async_copy(vis.at[:, :, :, columns], vis_v.at[slot], load_sem.at[slot])

    my_rows = pl.ds(pl.multiple_of(g * 16, 16), 16)
    my_columns = pl.ds(pl.multiple_of(g * 128, 128), 128)
    own = pltpu.make_async_copy(vis.at[:, :, :, my_columns], streams.at[:, :, my_rows, :], self_sem)
    loads = [load(slot, peer) for slot, peer in enumerate(peers)]
    for copy in loads:
        copy.start()
    own.start()
    proj_loads = [
        pltpu.make_async_copy(
            proj.at[:, n * CC : (n + 1) * CC], proj_v.at[:, n * CC : (n + 1) * CC], proj_sem.at[n]
        )
        for n in range(NC)
    ]
    pl.semaphore_wait(barrier, len(others))

    pending = []

    def a_copy(n, slot, peer):
        channels = pl.ds(n * CC, CC)
        return pltpu.make_async_remote_copy(
            src_ref=vis_v.at[slot, :, channels],
            dst_ref=streams.at[:, channels, my_rows, :],
            send_sem=a_ssem.at[n, slot],
            recv_sem=a_rsem.at[n, slot],
            device_id=plane_device(peer),
            device_id_type=MESH,
        )

    a_copies = [[a_copy(n, slot, peer) for slot, peer in enumerate(peers)] for n in range(NC)]
    for n in range(NC):
        for slot in range(len(peers)):
            if n == 0:
                loads[slot].wait()
            a_copies[n][slot].start()
            pending.append(a_copies[n][slot])
    for copy in proj_loads:
        copy.start()

    row = iota((256, 128), 0)
    lane = iota((256, 128), 1)
    slot_of_row = (row >> 5) * 16 + (row & 7) * 2 + ((row >> 4) & 1)
    order = jnp.sum(jnp.where(lane == slot_of_row, az[...], 0.0), axis=1, keepdims=True)
    row = iota((256, 256), 0)
    lane = iota((256, 256), 1)
    time = z * 128 + (lane & 127)
    quarter = (row >> 3) & 1
    phase = order.astype(jnp.int32) * time + 256 * quarter - 256 * (lane >> 7)
    values = cosine_of(phase & 1023) * F32(1.0 / 32.0)
    upper = values.astype(BF16)
    table[:, :256] = upper
    table[:, 256:] = (values - upper.astype(F32)).astype(BF16)

    chan = iota((64, 256), 0)
    col = iota((64, 256), 1)
    col_chan = (col >> 6) * 16 + ((col >> 4) & 3) * 4 + ((col >> 1) & 3)
    for s in range(2):
        hit = (chan == col_chan) & (((col >> 3) & 1) == s)
        even = jnp.where(hit & ((col & 1) == 0), 1.0, 0.0).astype(BF16)
        odd = jnp.where(hit & ((col & 1) == 1), 1.0, 0.0).astype(BF16)
        w_re, w_im = kl[s, 0], kl[s, 1]
        dot = functools.partial(jnp.dot, preferred_element_type=F32)
        klw[s * 128 : s * 128 + 64] = (dot(w_re, even) - dot(w_im, odd)).astype(BF16)
        klw[s * 128 + 64 : s * 128 + 128] = (dot(w_im, even) + dot(w_re, odd)).astype(BF16)

    def chain(n, forward):
        return 4 if (n % 2 == 0) == forward else 3

    def b_copy(n, way, i):
        return pltpu.make_async_remote_copy(
            src_ref=b_send.at[n, way, i],
            dst_ref=b_recv.at[n, way, i],
            send_sem=b_ssem.at[n, way, i],
            recv_sem=b_rsem.at[n, way, i],
            device_id=z_device(1 if way == 0 else -1),
            device_id_type=MESH,
        )

    def own_part(n, dz):
        plane = lax.rem(z + dz + 2 * ZN, ZN)
        return partial[n, pl.ds(pl.multiple_of(plane * 32, 32), 32), :]

    def dft(n):
        if n == 0:
            own.wait()
        for copy in a_copies[n]:
            copy.wait_recv()
        blocks = []
        for c in range(n * CC, (n + 1) * CC):
            both = jnp.concatenate([streams[0, c], streams[1, c]], axis=0)
            blocks.append(jnp.concatenate([both, both], axis=0))
        samples = jnp.concatenate(blocks, axis=1)
        partial[n] = jnp.dot(table[...], samples, preferred_element_type=F32)
        for way in range(2):
            length = chain(n, way == 0)
            b_send[n, way, 0] = own_part(n, length if way == 0 else -length).astype(BF16)
            copy = b_copy(n, way, 0)
            copy.start()
            pending.append(copy)

    def forward(n, i):
        for way in range(2):
            length = chain(n, way == 0)
            if i < length:
                b_copy(n, way, i - 1).wait_recv()
                left = length - i
                term = own_part(n, left if way == 0 else -left)
                b_send[n, way, i] = (b_recv[n, way, i - 1].astype(F32) + term).astype(BF16)
                copy = b_copy(n, way, i)
                copy.start()
                pending.append(copy)

    def c_copy(n, slot, peer):
        return pltpu.make_async_remote_copy(
            src_ref=c_send.at[n, peer],
            dst_ref=c_recv.at[n, g],
            send_sem=c_ssem.at[n, slot],
            recv_sem=c_rsem.at[n, slot],
            device_id=plane_device(peer),
            device_id_type=MESH,
        )

    def finish(n):
        total = own_part(n, 0)
        for way in range(2):
            last = chain(n, way == 0) - 1
            b_copy(n, way, last).wait_recv()
            total = total + b_recv[n, way, last].astype(F32)
        for s in range(2):
            for c in range(CC):
                for q in range(2):
                    at = ((s * CC + c) * 2 + q) * 8
                    rows = (s * 2 + q) * 8
                    final[n, at : at + 8, :] = total[rows : rows + 8, c * 128 : (c + 1) * 128]
        for peer in range(GN):
            c_send[n, peer] = final[n, pl.ds(peer, 16, stride=8), :].astype(BF16)
        for slot, peer in enumerate(peers):
            copy = c_copy(n, slot, peer)
            copy.start()
            pending.append(copy)
        c_recv[n, g] = c_send[n, g]

    def d_copy(n, dx):
        return pltpu.make_async_remote_copy(
            src_ref=d_recv.at[x, n],
            dst_ref=d_recv.at[x, n],
            send_sem=d_ssem.at[n, dx - 1],
            recv_sem=d_rsem.at[n, dx - 1],
            device_id=(tm, x_peer(dx)),
            device_id_type=MESH,
        )

    def project(n):
        proj_loads[n].wait()
        for slot, peer in enumerate(peers):
            c_copy(n, slot, peer).wait_recv()
        row = iota((16, 128), 0)
        lane = iota((16, 128), 1)
        wide_row = iota((16, 512), 0)
        raw = []
        live_count = []
        for p in range(2):
            vectors = jnp.concatenate([c_recv[n, 4 * p + j] for j in range(4)], axis=1)
            total = jnp.zeros((16, 128), F32)
            count = jnp.zeros((16, 128), jnp.int32)
            for s in range(2):
                for c in range(CC):
                    slot = s * CC + c
                    picked = jnp.where((wide_row >> 1) == slot, vectors, jnp.zeros_like(vectors))
                    matrix = proj_v[s, n * CC + c, p].reshape(128, 512)
                    total = total + lax.dot_general(
                        picked, matrix, (((1,), (1,)), ((), ())), preferred_element_type=F32
                    )
                    count = jnp.where((row >> 1) == slot, live[s, p, n * CC + c], count)
            raw.append(total)
            live_count.append(count)

        def swap_parts(v):
            return jnp.where((row & 1) == 0, pltpu.roll(v, 15, 0), pltpu.roll(v, 1, 0))

        sign = jnp.where((row & 1) == 0, -1.0, 1.0)
        low = raw[0] + sign * swap_parts(pltpu.roll(raw[0], 64, 1))
        high = pltpu.roll(raw[1], 64, 1) + sign * swap_parts(raw[1])
        modes = jnp.where(lane < 64, low, high)
        count = jnp.where(lane < 64, live_count[0], live_count[1])
        d_recv[x, n] = jnp.where((lane & 63) < count, modes, 0.0).astype(BF16)
        for dx in (1, 2, 3):
            copy = d_copy(n, dx)
            copy.start()
            pending.append(copy)

    for step in range(NC + 5):
        if step < NC:
            dft(step)
        for i in (1, 2, 3):
            if 0 <= step - i < NC:
                forward(step - i, i)
        if 0 <= step - 4 < NC:
            finish(step - 4)
        if 0 <= step - 5 < NC:
            project(step - 5)

    for n in range(NC):
        for dx in (1, 2, 3):
            d_copy(n, dx).wait_recv()
    gathered = d_recv[...].reshape(256, 128)
    for s in range(2):
        block = jnp.dot(klw[s * 128 : (s + 1) * 128], gathered, preferred_element_type=F32)
        mixed[s] = jnp.transpose(block)
        for p in range(2):
            rows = mixed[s, pl.ds(pl.multiple_of(p * 64 + x * 16, 16), 16), :]
            for q in range(2):
                out[s, q, p] = rows[:, q * 64 : (q + 1) * 64]
    for copy in pending:
        copy.wait_send()


def shards(visibilities, projection, kl_weight, azimuthal, live_mode_totals):
    hbm = pl.BlockSpec(memory_space=pl.ANY)
    vmem = pl.BlockSpec(memory_space=pltpu.VMEM)
    smem = pl.BlockSpec(memory_space=pltpu.SMEM)
    dma = pltpu.SemaphoreType.DMA
    out = pl.pallas_call(
        kernel,
        out_shape=jax.ShapeDtypeStruct((2, 2, 2, 16, 64), F32),
        in_specs=[hbm, hbm, vmem, vmem, smem],
        out_specs=vmem,
        scratch_shapes=[
            pltpu.VMEM((7, 2, 16, 16, 128), BF16),
            pltpu.VMEM((2, 16, 128, 128), BF16),
            pltpu.VMEM((2, 16, 2, 2, 64, 512), BF16),
            pltpu.VMEM((256, 512), BF16),
            pltpu.VMEM((NC, 256, 512), F32),
            pltpu.VMEM((NC, 2, 4, 32, 512), BF16),
            pltpu.VMEM((NC, 2, 4, 32, 512), BF16),
            pltpu.VMEM((NC, 128, 128), F32),
            pltpu.VMEM((NC, GN, 16, 128), BF16),
            pltpu.VMEM((NC, GN, 16, 128), BF16),
            pltpu.VMEM((XN, NC, 16, 128), BF16),
            pltpu.VMEM((256, 256), BF16),
            pltpu.VMEM((2, 128, 128), F32),
            dma((7,)),
            dma,
            dma((NC,)),
            dma((NC, 7)),
            dma((NC, 7)),
            dma((NC, 2, 4)),
            dma((NC, 2, 4)),
            dma((NC, 7)),
            dma((NC, 7)),
            dma((NC, 3)),
            dma((NC, 3)),
        ],
        compiler_params=pltpu.CompilerParams(
            collective_id=0, has_side_effects=True, vmem_limit_bytes=48 * 1024 * 1024
        ),
        name="mmode",
    )(
        visibilities,
        projection,
        kl_weight,
        azimuthal.astype(F32).reshape(1, 128),
        jnp.transpose(live_mode_totals, (0, 2, 1)),
    )
    return jnp.transpose(out, (0, 1, 4, 2, 3))


def solution(mesh):
    return jax.shard_map(
        shards,
        mesh=mesh,
        in_specs=(
            P(None, "freq", "tm", None),
            P("tm", "freq", None, None, None, None),
            P("tm", None, None, None),
            P(),
            P("tm", "freq", None),
        ),
        out_specs=P("tm", None, None, None, "freq"),
        check_vma=False,
    )
```

```python
import functools
import math

import jax
import jax.numpy as jnp
from jax import lax
from jax.experimental import pallas as pl
from jax.experimental.pallas import tpu as pltpu
from jax.sharding import PartitionSpec as P

MESH = pl.DeviceIdType.MESH
F32 = jnp.float32
BF16 = jnp.bfloat16

ZN = 8
GN = 8
XN = 4
NC = 4
CC = 4
NH = 8
HC = 2
WAYS = ((0, 1), (1, -1))
CHAINS = 3
FIRST, NEXT, HOP, FAR, CROSS = 7.0, 1.35, 3.0, 3.6, 3.4
SENDS = ((1, 0), (3, 0), (2, 0), (0, 1), (1, 1), (3, 1), (2, 1))


def iota(shape, dim):
    return lax.broadcasted_iota(jnp.int32, shape, dim)


def cosine_of(phase):
    angle = (jnp.abs(phase - 512) - 256).astype(F32) * (2.0 * math.pi / 1024)
    square = angle * angle
    series = F32(1.0 / math.factorial(13))
    for order in (11, 9, 7, 5, 3, 1):
        sign = 1.0 if (order // 2) % 2 == 0 else -1.0
        series = series * square + F32(sign / math.factorial(order))
    return series * angle


def kernel(
    vis, proj, kl_hbm, az_hbm, live_hbm, out,
    kl, az, live, vis_v, streams, proj_v, table, partial, b_send, b_recv, final, c_send, c_recv, d_recv, klw, mixed,
    small_sem, load_sem, self_sem, proj_sem, a_ssem, a_rsem, b_ssem, b_rsem, c_ssem, c_rsem, d_ssem, d_rsem,
):
    tm = lax.axis_index("tm")
    x = lax.axis_index("freq")
    z = tm // GN
    g = lax.rem(tm, GN)
    y = g // 2
    core = lax.rem(g, 2)

    def in_plane(dy, dc):
        return lax.rem(y + dy, 4) * 2 + lax.rem(core + dc, 2)

    def plane_device(peer):
        return (z * GN + peer, x)

    def z_device(dz):
        return (lax.rem(z + dz + ZN, ZN) * GN + g, x)

    def x_peer(dx):
        return lax.rem(x + dx, XN)

    peers = [in_plane(dy, dc) for dy, dc in SENDS]
    others = [plane_device(peer) for peer in peers]
    others += [z_device(1), z_device(-1), z_device(2), z_device(-2)]
    others += [(tm, x_peer(dx)) for dx in (1, 2, 3)]

    barrier = pltpu.get_barrier_semaphore()
    for device in others:
        pl.semaphore_signal(barrier, inc=1, device_id=device, device_id_type=MESH)

    def load(slot, block):
        columns = pl.ds(pl.multiple_of(block * 128, 128), 128)
        return pltpu.make_async_copy(vis.at[:, :, :, columns], vis_v.at[slot], load_sem.at[slot])

    my_rows = pl.ds(pl.multiple_of(g * 16, 16), 16)
    my_columns = pl.ds(pl.multiple_of(g * 128, 128), 128)
    own = pltpu.make_async_copy(vis.at[:, :, :, my_columns], streams.at[:, :, my_rows, :], self_sem)
    loads = [load(slot, peer) for slot, peer in enumerate(peers)]
    smalls = [
        pltpu.make_async_copy(source, target, small_sem.at[k])
        for k, (source, target) in enumerate(((az_hbm, az), (kl_hbm, kl), (live_hbm, live)))
    ]
    for copy in loads:
        copy.start()
    own.start()
    for copy in smalls:
        copy.start()
    proj_loads = [
        pltpu.make_async_copy(
            proj.at[:, n * CC : (n + 1) * CC], proj_v.at[:, n * CC : (n + 1) * CC], proj_sem.at[n]
        )
        for n in range(NC)
    ]
    with jax.named_scope("enter"):
        pl.semaphore_wait(barrier, len(others))

    def wait_bytes(sem, ref):
        pltpu.make_async_copy(ref, ref, sem).wait()

    def a_copy(n, slot, peer):
        channels = pl.ds(n * HC, HC)
        return pltpu.make_async_remote_copy(
            src_ref=vis_v.at[slot, :, channels],
            dst_ref=streams.at[:, channels, my_rows, :],
            send_sem=a_ssem,
            recv_sem=a_rsem.at[n],
            device_id=plane_device(peer),
            device_id_type=MESH,
        )

    a_copies = [[a_copy(n, slot, peer) for slot, peer in enumerate(peers)] for n in range(NH)]
    with jax.named_scope("send"):
        for n in range(NH):
            for slot in range(len(peers)):
                if n == 0:
                    loads[slot].wait()
                a_copies[n][slot].start()
        for copy in proj_loads:
            copy.start()

    for copy in smalls:
        copy.wait()
    row = iota((256, 128), 0)
    lane = iota((256, 128), 1)
    slot_of_row = (row >> 5) * 16 + (row & 7) * 2 + ((row >> 4) & 1)
    order = jnp.sum(jnp.where(lane == slot_of_row, az[...].astype(F32), 0.0), axis=1, keepdims=True)
    row = iota((256, 256), 0)
    lane = iota((256, 256), 1)
    time = z * 128 + (lane & 127)
    quarter = (row >> 3) & 1
    phase = order.astype(jnp.int32) * time + 256 * quarter - 256 * (lane >> 7)
    values = cosine_of(phase & 1023) * F32(1.0 / 32.0)
    upper = values.astype(BF16)
    table[:, :256] = upper
    table[:, 256:] = (values - upper.astype(F32)).astype(BF16)

    chan = iota((64, 256), 0)
    col = iota((64, 256), 1)
    col_chan = (col >> 6) * 16 + ((col >> 4) & 3) * 4 + ((col >> 1) & 3)
    for s in range(2):
        hit = (chan == col_chan) & (((col >> 3) & 1) == s)
        even = jnp.where(hit & ((col & 1) == 0), 1.0, 0.0).astype(BF16)
        odd = jnp.where(hit & ((col & 1) == 1), 1.0, 0.0).astype(BF16)
        w_re, w_im = kl[s, 0], kl[s, 1]
        dot = functools.partial(jnp.dot, preferred_element_type=F32)
        klw[s * 128 : s * 128 + 64] = (dot(w_re, even) - dot(w_im, odd)).astype(BF16)
        klw[s * 128 + 64 : s * 128 + 128] = (dot(w_im, even) + dot(w_re, odd)).astype(BF16)

    def chain(n, forward):
        return 4 if (n % 2 == 0) == forward else 3

    def b_start(n, slot, dz, value, group):
        b_send[n, slot] = value.astype(BF16)
        pltpu.make_async_remote_copy(
            src_ref=b_send.at[n, slot],
            dst_ref=b_recv.at[n, slot],
            send_sem=b_ssem,
            recv_sem=b_rsem.at[n, group],
            device_id=z_device(dz),
            device_id_type=MESH,
        ).start()

    def b_take(n, group, slots):
        wait_bytes(b_rsem.at[n, group], b_send.at[n, pl.ds(0, len(slots))])
        return [b_recv[n, slot].astype(F32) for slot in slots]

    def own_part(n, dz):
        plane = lax.rem(z + dz + 2 * ZN, ZN)
        return partial[n, pl.ds(pl.multiple_of(plane * 32, 32), 32), :]

    def dft(n):
        if n == 0:
            own.wait()
        wait_bytes(a_rsem.at[n], vis_v.at[:, :, pl.ds(n * HC, HC)])
        blocks = []
        for c in range(n * HC, (n + 1) * HC):
            both = jnp.concatenate([streams[0, c], streams[1, c]], axis=0)
            blocks.append(jnp.concatenate([both, both], axis=0))
        samples = jnp.concatenate(blocks, axis=1)
        partial[n] = jnp.dot(table[...], samples, preferred_element_type=F32)
        if n < CHAINS:
            for way, dz in WAYS:
                b_start(n, 4 * way, dz, own_part(n, dz * chain(n, way == 0)), 0)
        else:
            far = 2 if n % 2 == 0 else -2
            b_start(n, 2, far, own_part(n, 2 * far), 0)
            b_start(n, 0, 1, own_part(n, 3), 0)
            b_start(n, 1, -1, own_part(n, -3), 0)
            b_start(n, 3, 1, own_part(n, 1), 1)
            b_start(n, 4, -1, own_part(n, -1), 1)

    def forward(n, i):
        ways = [(way, dz) for way, dz in WAYS if chain(n, way == 0) > i]
        came = b_take(n, i - 1, [4 * way + i - 1 for way, _ in ways])
        for (way, dz), value in zip(ways, came, strict=True):
            left = chain(n, way == 0) - i
            b_start(n, 4 * way + i, dz, value + own_part(n, dz * left), 3 if left == 1 else i)

    def relay(n):
        came = b_take(n, 0, [0, 1, 2])
        came[n % 2] = came[n % 2] + came[2]
        for way, dz in WAYS:
            b_start(n, 5 + way, 2 * dz, came[way] + own_part(n, 2 * dz), 1)

    def last_slots(n):
        if n < CHAINS:
            return 3, [4 * way + chain(n, way == 0) - 1 for way, _ in WAYS]
        return 1, [3, 4, 5, 6]

    def c_copy(n, peer):
        return pltpu.make_async_remote_copy(
            src_ref=c_send.at[n, peer],
            dst_ref=c_recv.at[n, g],
            send_sem=c_ssem,
            recv_sem=c_rsem.at[n],
            device_id=plane_device(peer),
            device_id_type=MESH,
        )

    def finish(n):
        for half in range(2):
            h = 2 * n + half
            total = own_part(h, 0)
            for value in b_take(h, *last_slots(h)):
                total = total + value
            for s in range(2):
                for c in range(HC):
                    for q in range(2):
                        at = ((s * CC + half * HC + c) * 2 + q) * 8
                        rows = (s * 2 + q) * 8
                        final[n, at : at + 8, :] = total[rows : rows + 8, c * 128 : (c + 1) * 128]
        for peer in range(GN):
            c_send[n, peer] = final[n, pl.ds(peer, 16, stride=8), :].astype(BF16)
        for peer in peers:
            c_copy(n, peer).start()
        c_recv[n, g] = c_send[n, g]

    def d_copy(n, dx):
        return pltpu.make_async_remote_copy(
            src_ref=d_recv.at[x, n],
            dst_ref=d_recv.at[x, n],
            send_sem=d_ssem,
            recv_sem=d_rsem,
            device_id=(tm, x_peer(dx)),
            device_id_type=MESH,
        )

    def project(n):
        proj_loads[n].wait()
        wait_bytes(c_rsem.at[n], c_send.at[n, pl.ds(0, 7)])
        row = iota((16, 128), 0)
        lane = iota((16, 128), 1)
        wide_row = iota((16, 512), 0)
        raw = []
        live_count = []
        for p in range(2):
            vectors = jnp.concatenate([c_recv[n, 4 * p + j] for j in range(4)], axis=1)
            total = jnp.zeros((16, 128), F32)
            count = jnp.zeros((16, 128), jnp.int32)
            for s in range(2):
                for c in range(CC):
                    slot = s * CC + c
                    picked = jnp.where((wide_row >> 1) == slot, vectors, jnp.zeros_like(vectors))
                    matrix = proj_v[s, n * CC + c, p].reshape(128, 512)
                    total = total + lax.dot_general(
                        picked, matrix, (((1,), (1,)), ((), ())), preferred_element_type=F32
                    )
                    count = jnp.where((row >> 1) == slot, live[s, p, n * CC + c], count)
            raw.append(total)
            live_count.append(count)

        def swap_parts(v):
            return jnp.where((row & 1) == 0, pltpu.roll(v, 15, 0), pltpu.roll(v, 1, 0))

        sign = jnp.where((row & 1) == 0, -1.0, 1.0)
        low = raw[0] + sign * swap_parts(pltpu.roll(raw[0], 64, 1))
        high = pltpu.roll(raw[1], 64, 1) + sign * swap_parts(raw[1])
        modes = jnp.where(lane < 64, low, high)
        count = jnp.where(lane < 64, live_count[0], live_count[1])
        d_recv[x, n] = jnp.where((lane & 63) < count, modes, 0.0).astype(BF16)
        for dx in (1, 2, 3):
            d_copy(n, dx).start()

    tasks = []
    ready = []
    for h in range(NH):
        begin = FIRST + NEXT * h
        tasks.append((begin, f"dft{h}", functools.partial(dft, h)))
        if h < CHAINS:
            for i in (1, 2, 3):
                tasks.append((begin + HOP * i, f"fwd{h}_{i}", functools.partial(forward, h, i)))
            ready.append(begin + HOP * 4)
        else:
            tasks.append((begin + HOP, f"rel{h}", functools.partial(relay, h)))
            ready.append(begin + HOP + FAR)
    for n in range(NC):
        begin = max(ready[2 * n : 2 * n + 2])
        tasks.append((begin, f"fin{n}", functools.partial(finish, n)))
        tasks.append((begin + CROSS, f"prj{n}", functools.partial(project, n)))
    for _, name, task in sorted(tasks, key=lambda entry: entry[0]):
        with jax.named_scope(name):
            task()

    with jax.named_scope("dwait"):
        wait_bytes(d_rsem, d_recv.at[pl.ds(0, 3)])
    with jax.named_scope("mix"):
        gathered = d_recv[...].reshape(256, 128)
        for s in range(2):
            block = jnp.dot(klw[s * 128 : (s + 1) * 128], gathered, preferred_element_type=F32)
            mixed[s] = jnp.transpose(block)
            for p in range(2):
                rows = mixed[s, pl.ds(pl.multiple_of(p * 64 + x * 16, 16), 16), :]
                for q in range(2):
                    out[s, q, p] = rows[:, q * 64 : (q + 1) * 64]
    with jax.named_scope("drain"):
        wait_bytes(a_ssem, vis_v)
        wait_bytes(b_ssem, b_send.at[:, pl.ds(0, 7)])
        wait_bytes(c_ssem, c_send.at[:, pl.ds(0, 7)])
        wait_bytes(d_ssem, d_recv.at[pl.ds(0, 3)])


def shards(visibilities, projection, kl_weight, azimuthal, live_mode_totals):
    hbm = pl.BlockSpec(memory_space=pltpu.HBM)
    vmem = pl.BlockSpec(memory_space=pltpu.VMEM)
    dma = pltpu.SemaphoreType.DMA
    out = pl.pallas_call(
        kernel,
        out_shape=jax.ShapeDtypeStruct((2, 2, 2, 16, 64), F32),
        in_specs=[hbm] * 5,
        out_specs=vmem,
        scratch_shapes=[
            pltpu.VMEM((2, 2, 64, 64), BF16),
            pltpu.VMEM((1, 128), jnp.int32),
            pltpu.SMEM((2, 2, 16), jnp.int32),
            pltpu.VMEM((7, 2, 16, 16, 128), BF16),
            pltpu.VMEM((2, 16, 128, 128), BF16),
            pltpu.VMEM((2, 16, 2, 2, 64, 512), BF16),
            pltpu.VMEM((256, 512), BF16),
            pltpu.VMEM((NH, 256, 256), F32),
            pltpu.VMEM((NH, 8, 32, 256), BF16),
            pltpu.VMEM((NH, 8, 32, 256), BF16),
            pltpu.VMEM((NC, 128, 128), F32),
            pltpu.VMEM((NC, GN, 16, 128), BF16),
            pltpu.VMEM((NC, GN, 16, 128), BF16),
            pltpu.VMEM((XN, NC, 16, 128), BF16),
            pltpu.VMEM((256, 256), BF16),
            pltpu.VMEM((2, 128, 128), F32),
            dma((3,)),
            dma((7,)),
            dma,
            dma((NC,)),
            dma,
            dma((NH,)),
            dma,
            dma((NH, 4)),
            dma,
            dma((NC,)),
            dma,
            dma,
        ],
        compiler_params=pltpu.CompilerParams(
            collective_id=0, has_side_effects=True, vmem_limit_bytes=67043328
        ),
        name="mmode",
    )(
        visibilities,
        projection,
        kl_weight,
        azimuthal.reshape(1, 128),
        jnp.transpose(live_mode_totals, (0, 2, 1)),
    )
    return jnp.transpose(out, (0, 1, 4, 2, 3))


def solution(mesh):
    return jax.shard_map(
        shards,
        mesh=mesh,
        in_specs=(
            P(None, "freq", "tm", None),
            P("tm", "freq", None, None, None, None),
            P("tm", None, None, None),
            P(),
            P("tm", "freq", None),
        ),
        out_specs=P("tm", None, None, None, "freq"),
        check_vma=False,
    )
```

```python
import functools
import math

import jax
import jax.numpy as jnp
from jax import lax
from jax.experimental import pallas as pl
from jax.experimental.pallas import tpu as pltpu
from jax.sharding import PartitionSpec as P

MESH = pl.DeviceIdType.MESH
F32 = jnp.float32
BF16 = jnp.bfloat16

ZN = 8
GN = 8
XN = 4
NC = 4
CC = 4
NH = 8
HC = 2
WAYS = ((0, 1), (1, -1))
CHAIN, TRIPLE, PAIRS = 3, 2, 1
KINDS = (TRIPLE, TRIPLE, TRIPLE, TRIPLE, PAIRS, PAIRS, PAIRS, PAIRS)
SENDS = ((1, 0), (3, 0), (2, 0), (0, 1), (1, 1), (3, 1), (2, 1))
ORDER = ('dft0', 'dft1', 'dft2', 'dft3', 'fwd0_1', 'dft4', 'fwd1_1', 'dft5', 'fwd2_1', 'dft6', 'fwd3_1', 'fwd0_2', 'dft7', 'fwd4_1', 'fwd1_2', 'fwd5_1', 'fwd2_2', 'fwd6_1', 'fwd3_2', 'fwd7_1', 'fin0', 'fin2', 'fin1', 'fin3', 'prj0', 'prj2', 'prj1', 'prj3')


def iota(shape, dim):
    return lax.broadcasted_iota(jnp.int32, shape, dim)


def cosine_of(phase):
    angle = (jnp.abs(phase - 512) - 256).astype(F32) * (2.0 * math.pi / 1024)
    square = angle * angle
    series = F32(1.0 / math.factorial(13))
    for order in (11, 9, 7, 5, 3, 1):
        sign = 1.0 if (order // 2) % 2 == 0 else -1.0
        series = series * square + F32(sign / math.factorial(order))
    return series * angle


def kernel(
    vis, proj, kl_hbm, az_hbm, live_hbm, out,
    kl, az, live, vis_v, streams, proj_v, table, partial, b_send, b_recv, final, c_send, c_recv, d_recv, klw, mixed,
    small_sem, load_sem, self_sem, proj_sem, a_ssem, a_rsem, b_ssem, b_rsem, c_ssem, c_rsem, d_ssem, d_rsem,
):
    tm = lax.axis_index("tm")
    x = lax.axis_index("freq")
    z = tm // GN
    g = lax.rem(tm, GN)
    y = g // 2
    core = lax.rem(g, 2)

    def in_plane(dy, dc):
        return lax.rem(y + dy, 4) * 2 + lax.rem(core + dc, 2)

    def plane_device(peer):
        return (z * GN + peer, x)

    def z_device(dz):
        return (lax.rem(z + dz + ZN, ZN) * GN + g, x)

    def x_peer(dx):
        return lax.rem(x + dx, XN)

    peers = [in_plane(dy, dc) for dy, dc in SENDS]
    others = [plane_device(peer) for peer in peers]
    others += [z_device(1), z_device(-1), z_device(2), z_device(-2)]
    others += [(tm, x_peer(dx)) for dx in (1, 2, 3)]

    barrier = pltpu.get_barrier_semaphore()
    for device in others:
        pl.semaphore_signal(barrier, inc=1, device_id=device, device_id_type=MESH)

    def load(slot, block):
        columns = pl.ds(pl.multiple_of(block * 128, 128), 128)
        return pltpu.make_async_copy(vis.at[:, :, :, columns], vis_v.at[slot], load_sem.at[slot])

    my_rows = pl.ds(pl.multiple_of(g * 16, 16), 16)
    my_columns = pl.ds(pl.multiple_of(g * 128, 128), 128)
    own = pltpu.make_async_copy(vis.at[:, :, :, my_columns], streams.at[:, :, my_rows, :], self_sem)
    loads = [load(slot, peer) for slot, peer in enumerate(peers)]
    smalls = [
        pltpu.make_async_copy(source, target, small_sem.at[k])
        for k, (source, target) in enumerate(((az_hbm, az), (kl_hbm, kl), (live_hbm, live)))
    ]
    for copy in loads:
        copy.start()
    own.start()
    for copy in smalls:
        copy.start()
    proj_loads = [
        pltpu.make_async_copy(
            proj.at[:, n * CC : (n + 1) * CC], proj_v.at[:, n * CC : (n + 1) * CC], proj_sem.at[n]
        )
        for n in range(NC)
    ]
    with jax.named_scope("enter"):
        pl.semaphore_wait(barrier, len(others))

    def wait_bytes(sem, ref):
        pltpu.make_async_copy(ref, ref, sem).wait()

    def a_copy(n, slot, peer):
        channels = pl.ds(n * HC, HC)
        return pltpu.make_async_remote_copy(
            src_ref=vis_v.at[slot, :, channels],
            dst_ref=streams.at[:, channels, my_rows, :],
            send_sem=a_ssem,
            recv_sem=a_rsem.at[n],
            device_id=plane_device(peer),
            device_id_type=MESH,
        )

    a_copies = [[a_copy(n, slot, peer) for slot, peer in enumerate(peers)] for n in range(NH)]
    with jax.named_scope("send"):
        for n in range(NH):
            for slot in range(len(peers)):
                if n == 0:
                    loads[slot].wait()
                a_copies[n][slot].start()
        for copy in proj_loads:
            copy.start()

    for copy in smalls:
        copy.wait()
    row = iota((256, 128), 0)
    lane = iota((256, 128), 1)
    slot_of_row = (row >> 5) * 16 + (row & 7) * 2 + ((row >> 4) & 1)
    order = jnp.sum(jnp.where(lane == slot_of_row, az[...].astype(F32), 0.0), axis=1, keepdims=True)
    row = iota((256, 256), 0)
    lane = iota((256, 256), 1)
    time = z * 128 + (lane & 127)
    quarter = (row >> 3) & 1
    phase = order.astype(jnp.int32) * time + 256 * quarter - 256 * (lane >> 7)
    values = cosine_of(phase & 1023) * F32(1.0 / 32.0)
    upper = values.astype(BF16)
    table[:, :256] = upper
    table[:, 256:] = (values - upper.astype(F32)).astype(BF16)

    chan = iota((64, 256), 0)
    col = iota((64, 256), 1)
    col_chan = (col >> 6) * 16 + ((col >> 4) & 3) * 4 + ((col >> 1) & 3)
    for s in range(2):
        hit = (chan == col_chan) & (((col >> 3) & 1) == s)
        even = jnp.where(hit & ((col & 1) == 0), 1.0, 0.0).astype(BF16)
        odd = jnp.where(hit & ((col & 1) == 1), 1.0, 0.0).astype(BF16)
        w_re, w_im = kl[s, 0], kl[s, 1]
        dot = functools.partial(jnp.dot, preferred_element_type=F32)
        klw[s * 128 : s * 128 + 64] = (dot(w_re, even) - dot(w_im, odd)).astype(BF16)
        klw[s * 128 + 64 : s * 128 + 128] = (dot(w_im, even) + dot(w_re, odd)).astype(BF16)

    def chain(n, forward):
        return 4 if (n % 2 == 0) == forward else 3

    def b_start(n, slot, dz, value, group):
        b_send[n, slot] = value.astype(BF16)
        pltpu.make_async_remote_copy(
            src_ref=b_send.at[n, slot],
            dst_ref=b_recv.at[n, slot],
            send_sem=b_ssem,
            recv_sem=b_rsem.at[n, group],
            device_id=z_device(dz),
            device_id_type=MESH,
        ).start()

    def b_take(n, group, slots):
        wait_bytes(b_rsem.at[n, group], b_send.at[n, pl.ds(0, len(slots))])
        return [b_recv[n, slot].astype(F32) for slot in slots]

    def own_part(n, dz):
        plane = lax.rem(z + dz + 2 * ZN, ZN)
        return partial[n, pl.ds(pl.multiple_of(plane * 32, 32), 32), :]

    def dft(n):
        if n == 0:
            own.wait()
        wait_bytes(a_rsem.at[n], vis_v.at[:, :, pl.ds(n * HC, HC)])
        blocks = []
        for c in range(n * HC, (n + 1) * HC):
            both = jnp.concatenate([streams[0, c], streams[1, c]], axis=0)
            blocks.append(jnp.concatenate([both, both], axis=0))
        samples = jnp.concatenate(blocks, axis=1)
        partial[n] = jnp.dot(table[...], samples, preferred_element_type=F32)
        if KINDS[n] == CHAIN:
            for way, dz in WAYS:
                b_start(n, 4 * way, dz, own_part(n, dz * chain(n, way == 0)), 0)
        else:
            far = 2 if n % 2 == 0 else -2
            b_start(n, 2, far, own_part(n, 2 * far), 0)
            b_start(n, 0, 1, own_part(n, 3), 0)
            b_start(n, 1, -1, own_part(n, -3), 0)
            if KINDS[n] == PAIRS:
                b_start(n, 3, 1, own_part(n, 1), 3)
                b_start(n, 4, -1, own_part(n, -1), 3)

    def forward(n, i):
        if KINDS[n] == CHAIN:
            ways = [(way, dz) for way, dz in WAYS if chain(n, way == 0) > i]
            came = b_take(n, i - 1, [4 * way + i - 1 for way, _ in ways])
            for (way, dz), value in zip(ways, came, strict=True):
                left = chain(n, way == 0) - i
                b_start(n, 4 * way + i, dz, value + own_part(n, dz * left), 3 if left == 1 else i)
        elif i == 1:
            came = b_take(n, 0, [0, 1, 2])
            came[n % 2] = came[n % 2] + came[2]
            for way, dz in WAYS:
                step, group = (2 * dz, 3) if KINDS[n] == PAIRS else (dz, 1)
                b_start(n, 5 + way, step, came[way] + own_part(n, 2 * dz), group)
        else:
            for (way, dz), value in zip(WAYS, b_take(n, 1, [5, 6]), strict=True):
                b_start(n, 3 + way, dz, value + own_part(n, dz), 3)

    def last_slots(n):
        if KINDS[n] == CHAIN:
            return 3, [4 * way + chain(n, way == 0) - 1 for way, _ in WAYS]
        return 3, [3, 4, 5, 6] if KINDS[n] == PAIRS else [3, 4]

    def c_copy(n, peer):
        return pltpu.make_async_remote_copy(
            src_ref=c_send.at[n, peer],
            dst_ref=c_recv.at[n, g],
            send_sem=c_ssem,
            recv_sem=c_rsem.at[n],
            device_id=plane_device(peer),
            device_id_type=MESH,
        )

    def finish(n):
        for half in range(2):
            h = 2 * n + half
            total = own_part(h, 0)
            for value in b_take(h, *last_slots(h)):
                total = total + value
            for s in range(2):
                for c in range(HC):
                    for q in range(2):
                        at = ((s * CC + half * HC + c) * 2 + q) * 8
                        rows = (s * 2 + q) * 8
                        final[n, at : at + 8, :] = total[rows : rows + 8, c * 128 : (c + 1) * 128]
        for peer in range(GN):
            c_send[n, peer] = final[n, pl.ds(peer, 16, stride=8), :].astype(BF16)
        for peer in peers:
            c_copy(n, peer).start()
        c_recv[n, g] = c_send[n, g]

    def d_copy(n, dx):
        return pltpu.make_async_remote_copy(
            src_ref=d_recv.at[x, n],
            dst_ref=d_recv.at[x, n],
            send_sem=d_ssem,
            recv_sem=d_rsem,
            device_id=(tm, x_peer(dx)),
            device_id_type=MESH,
        )

    def project(n):
        proj_loads[n].wait()
        wait_bytes(c_rsem.at[n], c_send.at[n, pl.ds(0, 7)])
        row = iota((16, 128), 0)
        lane = iota((16, 128), 1)
        raw = []
        live_count = []
        for p in range(2):
            vectors = jnp.concatenate([c_recv[n, 4 * p + j] for j in range(4)], axis=1)
            total = jnp.zeros((16, 128), F32)
            count = jnp.zeros((16, 128), jnp.int32)
            for s in range(2):
                matrix = proj_v[s, n * CC : (n + 1) * CC, p].reshape(CC * 128, 512)
                products = lax.dot_general(
                    vectors, matrix, (((1,), (1,)), ((), ())), preferred_element_type=F32
                )
                for c in range(CC):
                    mine = (row >> 1) == s * CC + c
                    total = jnp.where(mine, products[:, c * 128 : (c + 1) * 128], total)
                    count = jnp.where(mine, live[s, p, n * CC + c], count)
            raw.append(total)
            live_count.append(count)

        def swap_parts(v):
            return jnp.where((row & 1) == 0, pltpu.roll(v, 15, 0), pltpu.roll(v, 1, 0))

        sign = jnp.where((row & 1) == 0, -1.0, 1.0)
        low = raw[0] + sign * swap_parts(pltpu.roll(raw[0], 64, 1))
        high = pltpu.roll(raw[1], 64, 1) + sign * swap_parts(raw[1])
        modes = jnp.where(lane < 64, low, high)
        count = jnp.where(lane < 64, live_count[0], live_count[1])
        d_recv[x, n] = jnp.where((lane & 63) < count, modes, 0.0).astype(BF16)
        for dx in (1, 2, 3):
            d_copy(n, dx).start()

    tasks = {}
    for h in range(NH):
        tasks[f"dft{h}"] = functools.partial(dft, h)
        for i in range(1, KINDS[h] + 1):
            tasks[f"fwd{h}_{i}"] = functools.partial(forward, h, i)
    for n in range(NC):
        tasks[f"fin{n}"] = functools.partial(finish, n)
        tasks[f"prj{n}"] = functools.partial(project, n)
    assert sorted(tasks) == sorted(ORDER)
    for name in ORDER:
        with jax.named_scope(name):
            tasks[name]()

    with jax.named_scope("dwait"):
        wait_bytes(d_rsem, d_recv.at[pl.ds(0, 3)])
    with jax.named_scope("mix"):
        gathered = d_recv[...].reshape(256, 128)
        for s in range(2):
            block = jnp.dot(klw[s * 128 : (s + 1) * 128], gathered, preferred_element_type=F32)
            mixed[s] = jnp.transpose(block)
            for p in range(2):
                rows = mixed[s, pl.ds(pl.multiple_of(p * 64 + x * 16, 16), 16), :]
                for q in range(2):
                    out[s, q, p] = rows[:, q * 64 : (q + 1) * 64]
    with jax.named_scope("drain"):
        wait_bytes(a_ssem, vis_v)
        wait_bytes(b_ssem, b_send.at[:, pl.ds(0, 7)])
        wait_bytes(c_ssem, c_send.at[:, pl.ds(0, 7)])
        wait_bytes(d_ssem, d_recv.at[pl.ds(0, 3)])


def shards(visibilities, projection, kl_weight, azimuthal, live_mode_totals):
    hbm = pl.BlockSpec(memory_space=pltpu.HBM)
    vmem = pl.BlockSpec(memory_space=pltpu.VMEM)
    dma = pltpu.SemaphoreType.DMA
    keep = functools.partial(pltpu.with_memory_space_constraint, memory_space=pltpu.HBM)
    out = pl.pallas_call(
        kernel,
        out_shape=jax.ShapeDtypeStruct((2, 2, 2, 16, 64), F32),
        in_specs=[hbm] * 5,
        out_specs=vmem,
        scratch_shapes=[
            pltpu.VMEM((2, 2, 64, 64), BF16),
            pltpu.VMEM((1, 128), jnp.int32),
            pltpu.SMEM((2, 2, 16), jnp.int32),
            pltpu.VMEM((7, 2, 16, 16, 128), BF16),
            pltpu.VMEM((2, 16, 128, 128), BF16),
            pltpu.VMEM((2, 16, 2, 2, 64, 512), BF16),
            pltpu.VMEM((256, 512), BF16),
            pltpu.VMEM((NH, 256, 256), F32),
            pltpu.VMEM((NH, 8, 32, 256), BF16),
            pltpu.VMEM((NH, 8, 32, 256), BF16),
            pltpu.VMEM((NC, 128, 128), F32),
            pltpu.VMEM((NC, GN, 16, 128), BF16),
            pltpu.VMEM((NC, GN, 16, 128), BF16),
            pltpu.VMEM((XN, NC, 16, 128), BF16),
            pltpu.VMEM((256, 256), BF16),
            pltpu.VMEM((2, 128, 128), F32),
            dma((3,)),
            dma((7,)),
            dma,
            dma((NC,)),
            dma,
            dma((NH,)),
            dma,
            dma((NH, 4)),
            dma,
            dma((NC,)),
            dma,
            dma,
        ],
        compiler_params=pltpu.CompilerParams(
            collective_id=0, has_side_effects=True, vmem_limit_bytes=48 * 1024 * 1024
        ),
        name="mmode",
    )(
        keep(visibilities),
        keep(projection),
        keep(kl_weight),
        keep(azimuthal.reshape(1, 128)),
        keep(jnp.transpose(live_mode_totals, (0, 2, 1))),
    )
    return jnp.transpose(out, (0, 1, 4, 2, 3))


def solution(mesh):
    return jax.shard_map(
        shards,
        mesh=mesh,
        in_specs=(
            P(None, "freq", "tm", None),
            P("tm", "freq", None, None, None, None),
            P("tm", None, None, None),
            P(),
            P("tm", "freq", None),
        ),
        out_specs=P("tm", None, None, None, "freq"),
        check_vma=False,
    )
```

```python
import functools
import math

import jax
import jax.numpy as jnp
from jax import lax
from jax.experimental import pallas as pl
from jax.experimental.pallas import tpu as pltpu
from jax.sharding import PartitionSpec as P

MESH = pl.DeviceIdType.MESH
F32 = jnp.float32
BF16 = jnp.bfloat16

ZN = 8
GN = 8
XN = 4
NC = 4
CC = 4
NH = 8
HC = 2
WAYS = ((0, 1), (1, -1))
CHAIN, TRIPLE, PAIRS = 3, 2, 1
KINDS = (PAIRS, PAIRS, TRIPLE, TRIPLE, TRIPLE, TRIPLE, PAIRS, PAIRS)
SENDS = ((1, 0), (3, 0), (2, 0), (0, 1), (1, 1), (3, 1), (2, 1))
ORDER = ('pre0', 'pre1', 'pre2', 'dft0', 'pre3', 'dft1', 'dft2', 'dft3', 'fwd0_1', 'dft4', 'fwd1_1', 'dft5', 'fwd2_1', 'dft6', 'fwd3_1', 'dft7', 'fwd4_1', 'fin0', 'fwd2_2', 'fwd5_1', 'fwd6_1', 'fwd3_2', 'fwd7_1', 'fwd4_2', 'prj0', 'fwd5_2', 'fin1', 'fin3', 'fin2', 'prj1', 'prj3', 'prj2')


def iota(shape, dim):
    return lax.broadcasted_iota(jnp.int32, shape, dim)


def cosine_of(phase):
    angle = (jnp.abs(phase - 512) - 256).astype(F32) * (2.0 * math.pi / 1024)
    square = angle * angle
    series = F32(1.0 / math.factorial(13))
    for order in (11, 9, 7, 5, 3, 1):
        sign = 1.0 if (order // 2) % 2 == 0 else -1.0
        series = series * square + F32(sign / math.factorial(order))
    return series * angle


def kernel(
    vis, proj, kl_hbm, az_hbm, live_hbm, out,
    kl, az, live, vis_v, streams, proj_v, proj_t, table, partial, b_send, b_recv, final, c_send, c_recv, d_recv, klw, mixed,
    small_sem, load_sem, self_sem, proj_sem, a_ssem, a_rsem, b_ssem, b_rsem, c_ssem, c_rsem, d_ssem, d_rsem,
):
    tm = lax.axis_index("tm")
    x = lax.axis_index("freq")
    z = tm // GN
    g = lax.rem(tm, GN)
    y = g // 2
    core = lax.rem(g, 2)

    def in_plane(dy, dc):
        return lax.rem(y + dy, 4) * 2 + lax.rem(core + dc, 2)

    def plane_device(peer):
        return (z * GN + peer, x)

    def z_device(dz):
        return (lax.rem(z + dz + ZN, ZN) * GN + g, x)

    def x_peer(dx):
        return lax.rem(x + dx, XN)

    peers = [in_plane(dy, dc) for dy, dc in SENDS]
    others = [plane_device(peer) for peer in peers]
    others += [z_device(1), z_device(-1), z_device(2), z_device(-2)]
    others += [(tm, x_peer(dx)) for dx in (1, 2, 3)]

    barrier = pltpu.get_barrier_semaphore()
    for device in others:
        pl.semaphore_signal(barrier, inc=1, device_id=device, device_id_type=MESH)

    def load(slot, block):
        columns = pl.ds(pl.multiple_of(block * 128, 128), 128)
        return pltpu.make_async_copy(vis.at[:, :, :, columns], vis_v.at[slot], load_sem.at[slot])

    my_rows = pl.ds(pl.multiple_of(g * 16, 16), 16)
    my_columns = pl.ds(pl.multiple_of(g * 128, 128), 128)
    own = pltpu.make_async_copy(vis.at[:, :, :, my_columns], streams.at[:, :, my_rows, :], self_sem)
    loads = [load(slot, peer) for slot, peer in enumerate(peers)]
    smalls = [
        pltpu.make_async_copy(source, target, small_sem.at[k])
        for k, (source, target) in enumerate(((az_hbm, az), (kl_hbm, kl), (live_hbm, live)))
    ]
    for copy in loads:
        copy.start()
    own.start()
    for copy in smalls:
        copy.start()
    proj_loads = [
        pltpu.make_async_copy(
            proj.at[:, n * CC : (n + 1) * CC], proj_v.at[:, n * CC : (n + 1) * CC], proj_sem.at[n]
        )
        for n in range(NC)
    ]
    with jax.named_scope("enter"):
        pl.semaphore_wait(barrier, len(others))

    def wait_bytes(sem, ref):
        pltpu.make_async_copy(ref, ref, sem).wait()

    def a_copy(n, slot, peer):
        channels = pl.ds(n * HC, HC)
        return pltpu.make_async_remote_copy(
            src_ref=vis_v.at[slot, :, channels],
            dst_ref=streams.at[:, channels, my_rows, :],
            send_sem=a_ssem,
            recv_sem=a_rsem.at[n],
            device_id=plane_device(peer),
            device_id_type=MESH,
        )

    a_copies = [[a_copy(n, slot, peer) for slot, peer in enumerate(peers)] for n in range(NH)]
    with jax.named_scope("send"):
        for n in range(NH):
            for slot in range(len(peers)):
                if n == 0:
                    loads[slot].wait()
                a_copies[n][slot].start()
        for copy in proj_loads:
            copy.start()

    for copy in smalls:
        copy.wait()
    row = iota((256, 128), 0)
    lane = iota((256, 128), 1)
    slot_of_row = (row >> 5) * 16 + (row & 7) * 2 + ((row >> 4) & 1)
    order = jnp.sum(jnp.where(lane == slot_of_row, az[...].astype(F32), 0.0), axis=1, keepdims=True)
    row = iota((256, 256), 0)
    lane = iota((256, 256), 1)
    time = z * 128 + (lane & 127)
    quarter = (row >> 3) & 1
    phase = order.astype(jnp.int32) * time + 256 * quarter - 256 * (lane >> 7)
    values = cosine_of(phase & 1023) * F32(1.0 / 32.0)
    upper = values.astype(BF16)
    table[:, :256] = upper
    table[:, 256:] = (values - upper.astype(F32)).astype(BF16)

    chan = iota((64, 256), 0)
    col = iota((64, 256), 1)
    col_chan = (col >> 6) * 16 + ((col >> 4) & 3) * 4 + ((col >> 1) & 3)
    for s in range(2):
        hit = (chan == col_chan) & (((col >> 3) & 1) == s)
        even = jnp.where(hit & ((col & 1) == 0), 1.0, 0.0).astype(BF16)
        odd = jnp.where(hit & ((col & 1) == 1), 1.0, 0.0).astype(BF16)
        w_re, w_im = kl[s, 0], kl[s, 1]
        dot = functools.partial(jnp.dot, preferred_element_type=F32)
        klw[s * 128 : s * 128 + 64] = (dot(w_re, even) - dot(w_im, odd)).astype(BF16)
        klw[s * 128 + 64 : s * 128 + 128] = (dot(w_im, even) + dot(w_re, odd)).astype(BF16)

    def chain(n, forward):
        return 4 if (n % 2 == 0) == forward else 3

    def b_start(n, slot, dz, value, group):
        b_send[n, slot] = value.astype(BF16)
        pltpu.make_async_remote_copy(
            src_ref=b_send.at[n, slot],
            dst_ref=b_recv.at[n, slot],
            send_sem=b_ssem,
            recv_sem=b_rsem.at[n, group],
            device_id=z_device(dz),
            device_id_type=MESH,
        ).start()

    def b_take(n, group, slots):
        wait_bytes(b_rsem.at[n, group], b_send.at[n, pl.ds(0, len(slots))])
        return [b_recv[n, slot].astype(F32) for slot in slots]

    def own_part(n, dz):
        plane = lax.rem(z + dz + 2 * ZN, ZN)
        return partial[n, pl.ds(pl.multiple_of(plane * 32, 32), 32), :]

    def dft(n):
        if n == 0:
            own.wait()
        wait_bytes(a_rsem.at[n], vis_v.at[:, :, pl.ds(n * HC, HC)])
        blocks = []
        for c in range(n * HC, (n + 1) * HC):
            both = jnp.concatenate([streams[0, c], streams[1, c]], axis=0)
            blocks.append(jnp.concatenate([both, both], axis=0))
        samples = jnp.concatenate(blocks, axis=1)
        partial[n] = jnp.dot(table[...], samples, preferred_element_type=F32)
        if KINDS[n] == CHAIN:
            for way, dz in WAYS:
                b_start(n, 4 * way, dz, own_part(n, dz * chain(n, way == 0)), 0)
        else:
            far = 2 if n % 2 == 0 else -2
            b_start(n, 2, far, own_part(n, 2 * far), 0)
            b_start(n, 0, 1, own_part(n, 3), 0)
            b_start(n, 1, -1, own_part(n, -3), 0)
            if KINDS[n] == PAIRS:
                b_start(n, 3, 1, own_part(n, 1), 3)
                b_start(n, 4, -1, own_part(n, -1), 3)

    def forward(n, i):
        if KINDS[n] == CHAIN:
            ways = [(way, dz) for way, dz in WAYS if chain(n, way == 0) > i]
            came = b_take(n, i - 1, [4 * way + i - 1 for way, _ in ways])
            for (way, dz), value in zip(ways, came, strict=True):
                left = chain(n, way == 0) - i
                b_start(n, 4 * way + i, dz, value + own_part(n, dz * left), 3 if left == 1 else i)
        elif i == 1:
            came = b_take(n, 0, [0, 1, 2])
            came[n % 2] = came[n % 2] + came[2]
            for way, dz in WAYS:
                step, group = (2 * dz, 3) if KINDS[n] == PAIRS else (dz, 1)
                b_start(n, 5 + way, step, came[way] + own_part(n, 2 * dz), group)
        else:
            for (way, dz), value in zip(WAYS, b_take(n, 1, [5, 6]), strict=True):
                b_start(n, 3 + way, dz, value + own_part(n, dz), 3)

    def last_slots(n):
        if KINDS[n] == CHAIN:
            return 3, [4 * way + chain(n, way == 0) - 1 for way, _ in WAYS]
        return 3, [3, 4, 5, 6] if KINDS[n] == PAIRS else [3, 4]

    def c_copy(n, peer):
        return pltpu.make_async_remote_copy(
            src_ref=c_send.at[n, peer],
            dst_ref=c_recv.at[n, g],
            send_sem=c_ssem,
            recv_sem=c_rsem.at[n],
            device_id=plane_device(peer),
            device_id_type=MESH,
        )

    def finish(n):
        for half in range(2):
            h = 2 * n + half
            total = own_part(h, 0)
            for value in b_take(h, *last_slots(h)):
                total = total + value
            for s in range(2):
                for c in range(HC):
                    for q in range(2):
                        at = ((s * CC + half * HC + c) * 2 + q) * 8
                        rows = (s * 2 + q) * 8
                        final[n, at : at + 8, :] = total[rows : rows + 8, c * 128 : (c + 1) * 128]
        for peer in range(GN):
            c_send[n, peer] = final[n, pl.ds(peer, 16, stride=8), :].astype(BF16)
        for peer in peers:
            c_copy(n, peer).start()
        c_recv[n, g] = c_send[n, g]

    def d_copy(n, dx):
        return pltpu.make_async_remote_copy(
            src_ref=d_recv.at[x, n],
            dst_ref=d_recv.at[x, n],
            send_sem=d_ssem,
            recv_sem=d_rsem,
            device_id=(tm, x_peer(dx)),
            device_id_type=MESH,
        )

    def prepare(n):
        proj_loads[n].wait()
        for s in range(2):
            for p in range(2):
                matrix = proj_v[s, n * CC : (n + 1) * CC, p].reshape(CC * 128, 512)
                proj_t[n, s, p] = jnp.transpose(matrix)

    def project(n):
        wait_bytes(c_rsem.at[n], c_send.at[n, pl.ds(0, 7)])
        row = iota((16, 128), 0)
        lane = iota((16, 128), 1)
        raw = []
        live_count = []
        for p in range(2):
            vectors = jnp.concatenate([c_recv[n, 4 * p + j] for j in range(4)], axis=1)
            total = jnp.zeros((16, 128), F32)
            count = jnp.zeros((16, 128), jnp.int32)
            for s in range(2):
                products = jnp.dot(vectors, proj_t[n, s, p], preferred_element_type=F32)
                for c in range(CC):
                    mine = (row >> 1) == s * CC + c
                    total = jnp.where(mine, products[:, c * 128 : (c + 1) * 128], total)
                    count = jnp.where(mine, live[s, p, n * CC + c], count)
            raw.append(total)
            live_count.append(count)

        def swap_parts(v):
            return jnp.where((row & 1) == 0, pltpu.roll(v, 15, 0), pltpu.roll(v, 1, 0))

        sign = jnp.where((row & 1) == 0, -1.0, 1.0)
        low = raw[0] + sign * swap_parts(pltpu.roll(raw[0], 64, 1))
        high = pltpu.roll(raw[1], 64, 1) + sign * swap_parts(raw[1])
        modes = jnp.where(lane < 64, low, high)
        count = jnp.where(lane < 64, live_count[0], live_count[1])
        d_recv[x, n] = jnp.where((lane & 63) < count, modes, 0.0).astype(BF16)
        for dx in (1, 2, 3):
            d_copy(n, dx).start()

    tasks = {}
    for h in range(NH):
        tasks[f"dft{h}"] = functools.partial(dft, h)
        for i in range(1, KINDS[h] + 1):
            tasks[f"fwd{h}_{i}"] = functools.partial(forward, h, i)
    for n in range(NC):
        tasks[f"fin{n}"] = functools.partial(finish, n)
        tasks[f"prj{n}"] = functools.partial(project, n)
        tasks[f"pre{n}"] = functools.partial(prepare, n)
    assert sorted(tasks) == sorted(ORDER)
    for name in ORDER:
        with jax.named_scope(name):
            tasks[name]()

    with jax.named_scope("dwait"):
        wait_bytes(d_rsem, d_recv.at[pl.ds(0, 3)])
    with jax.named_scope("mix"):
        gathered = d_recv[...].reshape(256, 128)
        for s in range(2):
            block = jnp.dot(klw[s * 128 : (s + 1) * 128], gathered, preferred_element_type=F32)
            mixed[s] = jnp.transpose(block)
            for p in range(2):
                rows = mixed[s, pl.ds(pl.multiple_of(p * 64 + x * 16, 16), 16), :]
                for q in range(2):
                    out[s, q, p] = rows[:, q * 64 : (q + 1) * 64]
    with jax.named_scope("drain"):
        wait_bytes(a_ssem, vis_v)
        wait_bytes(b_ssem, b_send.at[:, pl.ds(0, 7)])
        wait_bytes(c_ssem, c_send.at[:, pl.ds(0, 7)])
        wait_bytes(d_ssem, d_recv.at[pl.ds(0, 3)])


def shards(visibilities, projection, kl_weight, azimuthal, live_mode_totals):
    hbm = pl.BlockSpec(memory_space=pltpu.HBM)
    vmem = pl.BlockSpec(memory_space=pltpu.VMEM)
    dma = pltpu.SemaphoreType.DMA
    keep = functools.partial(pltpu.with_memory_space_constraint, memory_space=pltpu.HBM)
    out = pl.pallas_call(
        kernel,
        out_shape=jax.ShapeDtypeStruct((2, 2, 2, 16, 64), F32),
        in_specs=[hbm] * 5,
        out_specs=vmem,
        scratch_shapes=[
            pltpu.VMEM((2, 2, 64, 64), BF16),
            pltpu.VMEM((1, 128), jnp.int32),
            pltpu.SMEM((2, 2, 16), jnp.int32),
            pltpu.VMEM((7, 2, 16, 16, 128), BF16),
            pltpu.VMEM((2, 16, 128, 128), BF16),
            pltpu.VMEM((2, 16, 2, 2, 64, 512), BF16),
            pltpu.VMEM((NC, 2, 2, 512, 512), BF16),
            pltpu.VMEM((256, 512), BF16),
            pltpu.VMEM((NH, 256, 256), F32),
            pltpu.VMEM((NH, 8, 32, 256), BF16),
            pltpu.VMEM((NH, 8, 32, 256), BF16),
            pltpu.VMEM((NC, 128, 128), F32),
            pltpu.VMEM((NC, GN, 16, 128), BF16),
            pltpu.VMEM((NC, GN, 16, 128), BF16),
            pltpu.VMEM((XN, NC, 16, 128), BF16),
            pltpu.VMEM((256, 256), BF16),
            pltpu.VMEM((2, 128, 128), F32),
            dma((3,)),
            dma((7,)),
            dma,
            dma((NC,)),
            dma,
            dma((NH,)),
            dma,
            dma((NH, 4)),
            dma,
            dma((NC,)),
            dma,
            dma,
        ],
        compiler_params=pltpu.CompilerParams(
            collective_id=0, has_side_effects=True, vmem_limit_bytes=48 * 1024 * 1024
        ),
        name="mmode",
    )(
        keep(visibilities),
        keep(projection),
        keep(kl_weight),
        keep(azimuthal.reshape(1, 128)),
        keep(jnp.transpose(live_mode_totals, (0, 2, 1))),
    )
    return jnp.transpose(out, (0, 1, 4, 2, 3))


def solution(mesh):
    return jax.shard_map(
        shards,
        mesh=mesh,
        in_specs=(
            P(None, "freq", "tm", None),
            P("tm", "freq", None, None, None, None),
            P("tm", None, None, None),
            P(),
            P("tm", "freq", None),
        ),
        out_specs=P("tm", None, None, None, "freq"),
        check_vma=False,
    )
```
